32 devices in a mesh: samp: 16 (over z, y, x), tile: 2 (over core).
Axes of the slice: x: 2, y: 2, z: 4, core: 2. Of those that a mesh axis runs over, the one named last changes fastest.
Arguments:
- traits: bfloat16 [16384, 1024], P('samp'), may hold values from -300 to 300
- covariates: bfloat16 [16384, 32], P('samp'), may hold values from -6 to 6
- genotypes: int32 [16384, 512], P('samp', 'tile'), may hold values from 0 to 2
- shuffles: int32 [6, 16384], P(None, 'samp'), may hold values from 0 to 16383, as said below
Outputs:
- observed: float32 [1024, 512], P('samp', 'tile')
- perm_max: float32 [6, 1024], P(None, 'samp')
The draws below stay inside these ranges and needn't reach their ends.
Inputs may be any that keep to these rules, and one draw needn't show every extreme that they name: Row p of shuffles maps each aligned block of 1024 samples one to one onto the same block's samples.
All inputs are finite; a program needn't handle non-finite values.
Results may differ from the reference program's by a relative error of at most 0.0045.
Values sent between devices are 32-bit elements; how exact they have to be, the bound alone decides.
A program may use at most 64 MiB of HBM per device.

```python
import math
import jax
import jax.numpy as jnp
from jax import lax

SAMP_DEV = 1024
E = 1024
C = 32
PERMS = 6
SAMPLES = 16384
VARIANTS = 512


def covariate_base(key):
    values = jax.random.normal(jax.random.fold_in(key, 11), (SAMPLES, C), jnp.float32)
    return jnp.clip(values, -6.0, 6.0)


def draw_covariates(key, part):
    return covariate_base(key).astype(jnp.bfloat16)


def draw_traits(key, part):
    base = covariate_base(key)
    key_load, key_mean, key_noise, key_cols = jax.random.split(jax.random.fold_in(key, 23), 4)
    loading = jax.random.normal(key_load, (C, E), jnp.float32) / math.sqrt(C)
    means = 2.0 * jnp.clip(jax.random.normal(key_mean, (E,), jnp.float32), -4.0, 4.0)
    col_scale = jnp.exp(jax.random.uniform(key_cols, (E,), jnp.float32, 0.0, math.log(10.0)))
    position = jnp.arange(SAMPLES, dtype=jnp.float32) / SAMPLES
    noise = jnp.clip(jax.random.normal(key_noise, (SAMPLES, E), jnp.float32), -5.0, 5.0)
    row_scale = 1.0 + 2.0 * position
    fitted = jnp.dot(base, loading, precision=lax.Precision.HIGHEST)
    values = (means[None, :] + fitted + noise) * row_scale[:, None] * col_scale[None, :]
    return jnp.clip(values, -300.0, 300.0).astype(jnp.bfloat16)


def draw_genotypes(key, part):
    key_freq, key_first, key_second = jax.random.split(jax.random.fold_in(key, 37), 3)
    freq = jax.random.randint(key_freq, (1, VARIANTS), 5, 96)
    first = (jax.random.randint(key_first, (SAMPLES, VARIANTS), 0, 100) < freq).astype(jnp.int32)
    second = (jax.random.randint(key_second, (SAMPLES, VARIANTS), 0, 100) < freq).astype(jnp.int32)
    return first + second


def draw_shuffles(key, part):
    blocks = SAMPLES // SAMP_DEV
    keys = jax.random.split(jax.random.fold_in(key, 41), PERMS * blocks)
    orders = jax.vmap(lambda one_key: jax.random.permutation(one_key, SAMP_DEV))(keys).astype(jnp.int32)
    offsets = jnp.arange(blocks, dtype=jnp.int32) * SAMP_DEV
    orders = orders.reshape(PERMS, blocks, SAMP_DEV) + offsets[None, :, None]
    return orders.reshape(PERMS, SAMPLES).astype(jnp.int32)


def setup_inputs(seed: int = 0) -> dict:
    key_of = jax.random.split(jax.random.key(seed), 5)
    return {
        "traits": draw_traits(jax.random.fold_in(key_of[4], 71), 0),
        "covariates": draw_covariates(jax.random.fold_in(key_of[4], 71), 0),
        "genotypes": draw_genotypes(jax.random.fold_in(key_of[4], 71), 0),
        "shuffles": draw_shuffles(jax.random.fold_in(key_of[4], 71), 0),
    }


epsilon = 1e-05

def cholesky_solve(factor, rhs):
    first = lax.linalg.triangular_solve(factor, rhs, left_side=True, lower=True)
    return lax.linalg.triangular_solve(factor, first, left_side=True, lower=True, transpose_a=True)

def reference(traits, covariates, genotypes, shuffles):
    ones = jnp.ones((covariates.shape[0], 1), jnp.bfloat16)
    design = jnp.concatenate([ones, covariates], axis=1)
    dosage = genotypes.astype(jnp.bfloat16)
    gram = jnp.dot(design.T.astype(jnp.float32), design.astype(jnp.float32), preferred_element_type=jnp.float32)
    xty = jnp.dot(design.T.astype(jnp.float32), traits.astype(jnp.float32), preferred_element_type=jnp.float32)
    xtg = jnp.dot(design.T.astype(jnp.float32), dosage.astype(jnp.float32), preferred_element_type=jnp.float32)
    factor = jnp.linalg.cholesky(gram)
    coef_traits = cholesky_solve(factor, xty).astype(jnp.bfloat16)
    coef_geno = cholesky_solve(factor, xtg).astype(jnp.bfloat16)
    resid_traits = traits.astype(jnp.float32) - jnp.dot(design.astype(jnp.float32), coef_traits.astype(jnp.float32), preferred_element_type=jnp.float32)
    resid_geno = dosage.astype(jnp.float32) - jnp.dot(design.astype(jnp.float32), coef_geno.astype(jnp.float32), preferred_element_type=jnp.float32)
    mean_traits = lax.optimization_barrier(jnp.sum(resid_traits * resid_traits, axis=0)) / SAMPLES
    mean_geno = lax.optimization_barrier(jnp.sum(resid_geno * resid_geno, axis=0)) / SAMPLES
    rt_rows = resid_traits.astype(jnp.bfloat16)
    rg_rows = resid_geno.astype(jnp.bfloat16)
    scale_traits = lax.rsqrt(mean_traits + epsilon)
    scale_geno = lax.rsqrt(mean_geno + epsilon)
    factor_z = math.sqrt(SAMPLES - C - 2) / SAMPLES

    def scores_of(trait_rows):
        cross = jnp.dot(trait_rows.T.astype(jnp.float32), rg_rows.astype(jnp.float32), preferred_element_type=jnp.float32)
        return cross * scale_traits[:, None] * scale_geno[None, :] * factor_z
    observed = scores_of(rt_rows)

    def one_perm(order):
        shuffled = jnp.take(rt_rows, order.astype(jnp.int32), axis=0)
        return lax.optimization_barrier(jnp.max(jnp.abs(scores_of(shuffled)), axis=1))
    perm_max = lax.map(one_perm, shuffles)
    return (observed, perm_max)
```

```python
import functools
import math

import jax
import jax.numpy as jnp
from jax import lax
from jax.experimental import pallas as pl
from jax.experimental.pallas import tpu as pltpu
from jax.sharding import PartitionSpec as P

MESH = pl.DeviceIdType.MESH
LANES = 128
F32, BF16 = jnp.float32, jnp.bfloat16
epsilon = 1e-05

ORDERS = ((2, 1, 0), (1, 2, 0))


def grid_of(groups):
    x = 4 if groups % 32 == 0 else 2
    y = 2
    return (groups // (x * y), y, x)


def enter(me, groups):
    barrier = pltpu.get_barrier_semaphore()
    for d in range(1, groups):
        pl.semaphore_signal(
            barrier, inc=1, device_id={"samp": lax.rem(me + d, groups)}, device_id_type=MESH
        )
    return barrier


def gram_kernel(
    groups, dt_ref, d_ref, t_ref, g_ref, out_ref, parts, landed, mine, full, send, recv, send2, recv2
):
    me = lax.axis_index("samp")
    rows = dt_ref.shape[0]
    barrier = enter(me, groups)
    quota = parts.shape[0] // groups
    tile = 0

    def put(block):
        nonlocal tile
        for c in range(block.shape[1] // LANES):
            for r in range(rows // 8):
                parts[tile] = block[8 * r : 8 * r + 8, LANES * c : LANES * c + LANES]
                tile += 1

    dt = dt_ref[...]
    put(jnp.dot(dt, t_ref[...], preferred_element_type=F32))
    put(jnp.dot(dt, g_ref[...].astype(F32).astype(BF16), preferred_element_type=F32))
    put(jnp.dot(dt, d_ref[...], preferred_element_type=F32))
    used = tile
    for i in range(used, parts.shape[0]):
        parts[i] = jnp.zeros((8, LANES), F32)
    pl.semaphore_wait(barrier, groups - 1)
    copies = []
    for d in range(1, groups):
        peer = lax.rem(me + d, groups)
        copy = pltpu.make_async_remote_copy(
            src_ref=parts.at[pl.ds(peer * quota, quota)],
            dst_ref=landed.at[d - 1],
            send_sem=send.at[d - 1],
            recv_sem=recv.at[d - 1],
            device_id={"samp": peer},
            device_id_type=MESH,
        )
        copy.start()
        copies.append(copy)
    total = parts[pl.ds(me * quota, quota)]
    for d in range(1, groups):
        copies[d - 1].wait_recv()
        total = total + landed[d - 1]
    mine[...] = total
    full[pl.ds(me * quota, quota)] = total
    for d in range(1, groups):
        peer = lax.rem(me + d, groups)
        copy = pltpu.make_async_remote_copy(
            src_ref=mine,
            dst_ref=full.at[pl.ds(me * quota, quota)],
            send_sem=send2.at[d - 1],
            recv_sem=recv2.at[d - 1],
            device_id={"samp": peer},
            device_id_type=MESH,
        )
        copy.start()
        copies.append(copy)
    for d in range(1, groups):
        copies[groups - 2 + d].wait_recv()
    for i in range(used):
        c, r = divmod(i, rows // 8)
        out_ref[8 * r : 8 * r + 8, LANES * c : LANES * c + LANES] = full[i]
    for copy in copies:
        copy.wait_send()


def cross_products(design_t, design, traits, genotypes, groups):
    rows = design_t.shape[0]
    width = traits.shape[1] + genotypes.shape[1] + design.shape[1]
    tiles = rows // 8 * (width // LANES)
    quota = -(-tiles // groups)
    vmem = pl.BlockSpec(memory_space=pltpu.VMEM)
    sems = pltpu.SemaphoreType.DMA((groups - 1,))
    return pl.pallas_call(
        functools.partial(gram_kernel, groups),
        out_shape=jax.ShapeDtypeStruct((rows, width), F32),
        in_specs=[vmem] * 4,
        out_specs=vmem,
        scratch_shapes=[
            pltpu.VMEM((quota * groups, 8, LANES), F32),
            pltpu.VMEM((groups - 1, quota, 8, LANES), F32),
            pltpu.VMEM((quota, 8, LANES), F32),
            pltpu.VMEM((quota * groups, 8, LANES), F32),
            sems,
            sems,
            sems,
            sems,
        ],
        compiler_params=pltpu.CompilerParams(collective_id=0, has_side_effects=True),
        name="gram",
    )(design_t, design, traits, genotypes)


def scan_kernel(
    dims, samples, d_ref, t_ref, g_ref, ct_ref, cg_ref, order_ref, score_ref, peak_ref, square_ref,
    rt, rg, moved, prod, squares, sq_send, sq_recv, send, recv, *bufs
):
    groups = dims[0] * dims[1] * dims[2]
    me = lax.axis_index("samp")
    here = (me // (dims[1] * dims[2]), lax.rem(me // dims[2], dims[1]), lax.rem(me, dims[2]))
    turns, n_parts = prod.shape[0], prod.shape[1]
    share, width = prod.shape[5], prod.shape[6]
    local, traits = t_ref.shape
    barrier = enter(me, groups)

    step = min(256, local)
    sq_t = jnp.zeros((1, traits), F32)
    sq_g = jnp.zeros((1, width), F32)
    for i in range(local // step):
        at = slice(i * step, (i + 1) * step)
        d = d_ref[at, :]
        resid = t_ref[at, :].astype(F32) - jnp.dot(d, ct_ref[...], preferred_element_type=F32)
        sq_t = sq_t + jnp.sum(resid * resid, axis=0, keepdims=True)
        rt[:, at] = resid.astype(BF16).T
        dose = g_ref[at, :].astype(F32)
        resid = dose - jnp.dot(d, cg_ref[...], preferred_element_type=F32)
        sq_g = sq_g + jnp.sum(resid * resid, axis=0, keepdims=True)
        rg[at, :] = resid.astype(BF16)
    squares[0] = jnp.zeros(squares.shape[1:], F32)
    n_t = traits // LANES
    for c in range(n_t):
        squares[0, c : c + 1, :] = sq_t[:, c * LANES : (c + 1) * LANES]
    for c in range(width // LANES):
        squares[0, n_t + c : n_t + c + 1, :] = sq_g[:, c * LANES : (c + 1) * LANES]
    pl.semaphore_wait(barrier, groups - 1)

    def square_copy(d):
        return pltpu.make_async_remote_copy(
            src_ref=squares.at[0],
            dst_ref=squares.at[d],
            send_sem=sq_send.at[d - 1],
            recv_sem=sq_recv.at[d - 1],
            device_id={"samp": lax.rem(me + d, groups)},
            device_id_type=MESH,
        )

    def spot(axis, d):
        j = lax.rem(here[axis] + d, dims[axis])
        at = list(here)
        at[axis] = j
        return j, (at[0] * dims[1] + at[1]) * dims[2] + at[2]

    def pick(axis, order, stage, j):
        left = [a for a in (0, 1, 2) if a not in order[:stage]]
        return tuple(j if a == axis else slice(None) for a in left)

    def source(k, p, stage):
        if stage == 0:
            return prod.at[k, p]
        return bufs[5 * p + 2 * stage - 1].at[k]

    def copies(k, p, stage):
        order = ORDERS[p]
        axis = order[stage]
        first = sum(dims[a] - 1 for a in order[:stage])
        out = []
        for d in range(1, dims[axis]):
            j, peer = spot(axis, d)
            out.append(
                pltpu.make_async_remote_copy(
                    src_ref=source(k, p, stage).at[pick(axis, order, stage, j)],
                    dst_ref=bufs[5 * p + 2 * stage].at[k, d - 1],
                    send_sem=send.at[k, p, first + d - 1],
                    recv_sem=recv.at[k, p, first + d - 1],
                    device_id={"samp": peer},
                    device_id_type=MESH,
                )
            )
        return out

    def begin(k, stage):
        for p in range(n_parts):
            for copy in copies(k, p, stage):
                copy.start()

    def collect(k, stage):
        for p in range(n_parts):
            order = ORDERS[p]
            axis = order[stage]
            for copy in copies(k, p, stage):
                copy.wait_recv()
            total = source(k, p, stage)[pick(axis, order, stage, here[axis])]
            for d in range(1, dims[axis]):
                total = total + bufs[5 * p + 2 * stage][k, d - 1]
            if stage < 2:
                bufs[5 * p + 2 * stage + 1][k] = total
            else:
                score_ref[k, p * share : (p + 1) * share, :] = total

    def multiply(k):
        order = order_ref[pl.ds(k, 1), :]
        for i in range(local // step):
            row = lax.broadcasted_iota(jnp.int32, (step, local), 0) + i * step
            hot = jnp.where(row == order, 1.0, 0.0).astype(BF16)
            moved[i * step : (i + 1) * step, :] = jnp.dot(
                hot, rg[...], preferred_element_type=F32
            ).astype(BF16)
        depth = traits // dims[0]
        for z in range(dims[0]):
            block = jnp.dot(
                rt[z * depth : (z + 1) * depth, :], moved[...], preferred_element_type=F32
            ).reshape(dims[1], dims[2], n_parts, share, width)
            for p in range(n_parts):
                prod[k, p, z] = block[:, :, p]

    def turn(t, carry):
        @pl.when(t < turns)
        def _():
            multiply(t)
            begin(t, 0)

        @pl.when(t == 0)
        def _():
            for d in range(1, groups):
                square_copy(d).start()

        for stage in range(3):
            k = t - 1 - stage

            @pl.when(jnp.logical_and(k >= 0, k < turns))
            def _():
                collect(k, stage)
                if stage < 2:
                    begin(k, stage + 1)

        return carry

    lax.fori_loop(0, turns + 3, turn, 0)

    total = squares[0]
    for d in range(1, groups):
        square_copy(d).wait_recv()
        total = total + squares[d]
    square_ref[...] = total
    gain = lax.rsqrt(total / samples + epsilon)
    gain = jnp.concatenate([gain[n_t + c : n_t + c + 1, :] for c in range(width // LANES)], axis=1)
    for k in range(turns):
        scaled = score_ref[k] * gain
        score_ref[k] = scaled
        peak_ref[k] = jnp.broadcast_to(
            jnp.max(jnp.abs(scaled), axis=1, keepdims=True), peak_ref.shape[1:]
        )

    def finish(k, carry):
        for p in range(n_parts):
            for stage in range(3):
                for copy in copies(k, p, stage):
                    copy.wait_send()
        return carry

    lax.fori_loop(0, turns, finish, 0)
    for d in range(1, groups):
        square_copy(d).wait_send()


def scan(design, traits, genotypes, coef_t, coef_g, orders, groups):
    dims = grid_of(groups)
    turns = orders.shape[0]
    local, n_traits = traits.shape
    width = genotypes.shape[1]
    own = n_traits // groups
    n_parts = len(ORDERS)
    share = own // n_parts
    bufs = []
    for order in ORDERS:
        left = [0, 1, 2]
        for stage, axis in enumerate(order):
            left.remove(axis)
            rest = tuple(dims[a] for a in left) + (share, width)
            bufs.append(pltpu.VMEM((turns, dims[axis] - 1) + rest, F32))
            if stage < 2:
                bufs.append(pltpu.VMEM((turns,) + rest, F32))
    hops = sum(n - 1 for n in dims)
    rows = -(-(n_traits + width) // (8 * LANES)) * 8
    vmem = pl.BlockSpec(memory_space=pltpu.VMEM)
    sems = pltpu.SemaphoreType.DMA((turns, n_parts, hops))
    flat = pltpu.SemaphoreType.DMA((groups - 1,))
    return pl.pallas_call(
        functools.partial(scan_kernel, dims, local * groups),
        out_shape=(
            jax.ShapeDtypeStruct((turns, own, width), F32),
            jax.ShapeDtypeStruct((turns, own, LANES), F32),
            jax.ShapeDtypeStruct((rows, LANES), F32),
        ),
        in_specs=[vmem] * 6,
        out_specs=(vmem, vmem, vmem),
        scratch_shapes=[
            pltpu.VMEM((n_traits, local), BF16),
            pltpu.VMEM((local, width), BF16),
            pltpu.VMEM((local, width), BF16),
            pltpu.VMEM((turns, n_parts) + dims + (share, width), F32),
            pltpu.VMEM((groups, rows, LANES), F32),
            flat,
            flat,
            sems,
            sems,
            *bufs,
        ],
        compiler_params=pltpu.CompilerParams(
            collective_id=1, has_side_effects=True, vmem_limit_bytes=60 * 1024 * 1024
        ),
        name="scan",
    )(design, traits, genotypes, coef_t, coef_g, orders)


def cholesky_solve(factor, rhs):
    first = lax.linalg.triangular_solve(factor, rhs, left_side=True, lower=True)
    return lax.linalg.triangular_solve(factor, first, left_side=True, lower=True, transpose_a=True)


def shards(traits, covariates, genotypes, shuffles):
    groups = lax.axis_size("samp")
    me = lax.axis_index("samp")
    local, n_traits = traits.shape
    width = genotypes.shape[1]
    samples = local * groups
    used = covariates.shape[1] + 1
    rows = -(-used // 16) * 16
    wide = -(-used // LANES) * LANES
    ones = jnp.ones((local, 1), BF16)
    design = jnp.concatenate([ones, covariates, jnp.zeros((local, wide - used), BF16)], axis=1)
    design_t = design[:, :rows].T
    sums = cross_products(design_t, design, traits, genotypes, groups)
    gram = sums[:used, n_traits + width : n_traits + width + used]
    coef = cholesky_solve(jnp.linalg.cholesky(gram), sums[:used, : n_traits + width]).astype(BF16)
    coef = jnp.pad(coef, ((0, wide - used), (0, 0)))
    own_order = shuffles - me * local
    orders = jnp.concatenate([jnp.arange(local, dtype=jnp.int32)[None], own_order], axis=0)
    scores, peaks, squares = scan(
        design, traits, genotypes, coef[:, :n_traits], coef[:, n_traits:], orders, groups
    )
    own = n_traits // groups
    mine = lax.dynamic_slice_in_dim(squares.reshape(-1), me * own, own, 0)
    gain = lax.rsqrt(mine / samples + epsilon) * (math.sqrt(samples - used - 1) / samples)
    observed = scores[0] * gain[:, None]
    perm_max = lax.pmax(peaks[1:, :, 0] * gain[None, :], "tile")
    return (observed, perm_max)


def solution(mesh):
    placed = (P("samp", None), P("samp", None), P("samp", "tile"), P(None, "samp"))
    return jax.shard_map(
        shards,
        mesh=mesh,
        in_specs=placed,
        out_specs=(P("samp", "tile"), P(None, "samp")),
        check_vma=False,
    )
```

```python
import functools
import math

import jax
import jax.numpy as jnp
from jax import lax
from jax.experimental import pallas as pl
from jax.experimental.pallas import tpu as pltpu
from jax.sharding import PartitionSpec as P

MESH = pl.DeviceIdType.MESH
LANES = 128
F32, BF16 = jnp.float32, jnp.bfloat16
epsilon = 1e-05

ORDERS = ((2, 1, 0), (1, 2, 0))


def grid_of(groups):
    x = 4 if groups % 32 == 0 else 2
    y = 2
    return (groups // (x * y), y, x)


def start_all(copies):
    for copy in copies:
        copy.start()
    return copies


def scan_kernel(
    dims, tiles, samples, used, t_ref, c_ref, g_ref, order_ref, score_ref, peak_ref,
    design, parts, landed, mine, full, rhs, coef, rt, rg, moved, prod, found, squares, column,
    peaks, sum_sems, sq_send, sq_recv, tile_send, tile_recv, send, recv, *bufs
):
    groups = dims[0] * dims[1] * dims[2]
    me = lax.axis_index("samp")
    my_tile = lax.axis_index("tile")
    here = (me // (dims[1] * dims[2]), lax.rem(me // dims[2], dims[1]), lax.rem(me, dims[2]))
    turns, n_parts = prod.shape[0], prod.shape[1]
    share, width = prod.shape[5], prod.shape[6]
    local, traits = t_ref.shape
    own = traits // groups
    rows = coef.shape[0]
    quota = parts.shape[0] // groups
    strips = -(-used // 8)

    barrier = pltpu.get_barrier_semaphore()
    for d in range(1, groups):
        pl.semaphore_signal(
            barrier, inc=1, device_id={"samp": lax.rem(me + d, groups)}, device_id_type=MESH
        )
    for d in range(1, tiles):
        pl.semaphore_signal(
            barrier, inc=1, device_id={"tile": lax.rem(my_tile + d, tiles)}, device_id_type=MESH
        )

    lane = lax.broadcasted_iota(jnp.int32, design.shape, 1)
    design[...] = jnp.where(lane == used - 1, 1.0, 0.0).astype(BF16)
    design[:, : used - 1] = c_ref[...]
    design_t = design[...].T
    slot = 0
    for block_ref in (t_ref, g_ref, design):
        block = block_ref[...]
        if block.dtype != BF16:
            block = block.astype(F32).astype(BF16)
        block = jnp.dot(design_t, block, preferred_element_type=F32)
        for c in range(block.shape[1] // LANES):
            for r in range(strips):
                parts[slot] = block[8 * r : 8 * r + 8, LANES * c : LANES * c + LANES]
                slot += 1
    for i in range(slot, parts.shape[0]):
        parts[i] = jnp.zeros((8, LANES), F32)
    pl.semaphore_wait(barrier, groups + tiles - 2)

    def sum_copy(d, source, target, stage):
        return pltpu.make_async_remote_copy(
            src_ref=source,
            dst_ref=target,
            send_sem=sum_sems.at[2 * stage, d - 1],
            recv_sem=sum_sems.at[2 * stage + 1, d - 1],
            device_id={"samp": lax.rem(me + d, groups)},
            device_id_type=MESH,
        )

    scattered = start_all(
        [
            sum_copy(
                d, parts.at[pl.ds(lax.rem(me + d, groups) * quota, quota)], landed.at[d - 1], 0
            )
            for d in range(1, groups)
        ]
    )
    total = parts[pl.ds(me * quota, quota)]
    for d in range(1, groups):
        scattered[d - 1].wait_recv()
        total = total + landed[d - 1]
    mine[...] = total
    full[pl.ds(me * quota, quota)] = total
    gathered = start_all(
        [sum_copy(d, mine, full.at[pl.ds(me * quota, quota)], 1) for d in range(1, groups)]
    )
    rhs[...] = jnp.zeros(rhs.shape, F32)
    for copy in gathered:
        copy.wait_recv()

    n_t, n_g = traits // LANES, width // LANES
    half = rows // 2
    for c in range(n_t + n_g):
        for r in range(strips):
            rhs[half + 8 * r : half + 8 * r + 8, LANES * c : LANES * c + LANES] = full[
                c * strips + r
            ]
    gram = jnp.concatenate([full[(n_t + n_g) * strips + r] for r in range(strips)], axis=0)
    sub = lax.broadcasted_iota(jnp.int32, gram.shape, 0)
    lane = lax.broadcasted_iota(jnp.int32, gram.shape, 1)
    gram = jnp.where(lane == sub + half, 1.0, gram)
    for j in range(used):
        row = gram[j : j + 1, :] * (1.0 / gram[j : j + 1, j : j + 1])
        gram = jnp.where(sub == j, row, gram - gram[:, j : j + 1] * row)
    inverse = jnp.where(lane >= half, gram, 0.0)
    coef[...] = jnp.zeros(coef.shape, BF16)
    coef[: 8 * strips, :] = jnp.dot(
        inverse, rhs[...], precision=lax.Precision.HIGHEST, preferred_element_type=F32
    ).astype(BF16)

    step = min(256, local)
    sq_t = jnp.zeros((1, traits), F32)
    sq_g = jnp.zeros((1, width), F32)
    for i in range(local // step):
        at = slice(i * step, (i + 1) * step)
        d = design[at, :]
        resid = t_ref[at, :].astype(F32) - jnp.dot(
            d, coef[:, :traits], preferred_element_type=F32
        )
        sq_t = sq_t + jnp.sum(resid * resid, axis=0, keepdims=True)
        rt[:, at] = resid.astype(BF16).T
        dose = g_ref[at, :].astype(F32)
        resid = dose - jnp.dot(d, coef[:, traits:], preferred_element_type=F32)
        sq_g = sq_g + jnp.sum(resid * resid, axis=0, keepdims=True)
        rg[at, :] = resid.astype(BF16)
    squares[0] = jnp.zeros(squares.shape[1:], F32)
    for c in range(n_t):
        squares[0, c : c + 1, :] = sq_t[:, c * LANES : (c + 1) * LANES]
    for c in range(n_g):
        squares[0, n_t + c : n_t + c + 1, :] = sq_g[:, c * LANES : (c + 1) * LANES]

    def square_copy(d):
        return pltpu.make_async_remote_copy(
            src_ref=squares.at[0],
            dst_ref=squares.at[d],
            send_sem=sq_send.at[d - 1],
            recv_sem=sq_recv.at[d - 1],
            device_id={"samp": lax.rem(me + d, groups)},
            device_id_type=MESH,
        )

    def spot(axis, d):
        j = lax.rem(here[axis] + d, dims[axis])
        at = list(here)
        at[axis] = j
        return j, (at[0] * dims[1] + at[1]) * dims[2] + at[2]

    def pick(axis, order, stage, j):
        left = [a for a in (0, 1, 2) if a not in order[:stage]]
        return tuple(j if a == axis else slice(None) for a in left)

    def source(k, p, stage):
        if stage == 0:
            return prod.at[k, p]
        return bufs[5 * p + 2 * stage - 1].at[k]

    def copies(k, p, stage):
        order = ORDERS[p]
        axis = order[stage]
        first = sum(dims[a] - 1 for a in order[:stage])
        out = []
        for d in range(1, dims[axis]):
            j, peer = spot(axis, d)
            out.append(
                pltpu.make_async_remote_copy(
                    src_ref=source(k, p, stage).at[pick(axis, order, stage, j)],
                    dst_ref=bufs[5 * p + 2 * stage].at[k, d - 1],
                    send_sem=send.at[k, p, first + d - 1],
                    recv_sem=recv.at[k, p, first + d - 1],
                    device_id={"samp": peer},
                    device_id_type=MESH,
                )
            )
        return out

    def begin(k, stage):
        for p in range(n_parts):
            for copy in copies(k, p, stage):
                copy.start()

    def collect(k, stage):
        for p in range(n_parts):
            order = ORDERS[p]
            axis = order[stage]
            for copy in copies(k, p, stage):
                copy.wait_recv()
            total = source(k, p, stage)[pick(axis, order, stage, here[axis])]
            for d in range(1, dims[axis]):
                total = total + bufs[5 * p + 2 * stage][k, d - 1]
            if stage < 2:
                bufs[5 * p + 2 * stage + 1][k] = total
            else:
                found[k, p * share : (p + 1) * share, :] = total

    def multiply(k):
        @pl.when(k == 0)
        def _():
            moved[...] = rg[...]

        @pl.when(k > 0)
        def _():
            order = order_ref[pl.ds(k - 1, 1), :] - me * local
            for i in range(local // step):
                row = lax.broadcasted_iota(jnp.int32, (step, local), 0) + i * step
                hot = jnp.where(row == order, 1.0, 0.0).astype(BF16)
                moved[i * step : (i + 1) * step, :] = jnp.dot(
                    hot, rg[...], preferred_element_type=F32
                ).astype(BF16)

        depth = traits // dims[0]
        for z in range(dims[0]):
            block = jnp.dot(
                rt[z * depth : (z + 1) * depth, :], moved[...], preferred_element_type=F32
            ).reshape(dims[1], dims[2], n_parts, share, width)
            for p in range(n_parts):
                prod[k, p, z] = block[:, :, p]

    def turn(t, carry):
        @pl.when(t < turns)
        def _():
            multiply(t)
            begin(t, 0)

        @pl.when(t == 0)
        def _():
            for d in range(1, groups):
                square_copy(d).start()

        for stage in range(3):
            k = t - 1 - stage

            @pl.when(jnp.logical_and(k >= 0, k < turns))
            def _():
                collect(k, stage)
                if stage < 2:
                    begin(k, stage + 1)

        return carry

    lax.fori_loop(0, turns + 3, turn, 0)

    total = squares[0]
    for d in range(1, groups):
        square_copy(d).wait_recv()
        total = total + squares[d]
    gain = lax.rsqrt(total / samples + epsilon)
    factor = math.sqrt(samples - used - 1) / samples
    gain_g = jnp.concatenate([gain[n_t + c : n_t + c + 1, :] for c in range(n_g)], axis=1)
    turned = gain.T
    pos = lax.broadcasted_iota(jnp.int32, turned.shape, 1)
    chosen = jnp.sum(
        jnp.where(pos == me * own // LANES, turned, 0.0), axis=1, keepdims=True
    )
    column[...] = jnp.broadcast_to(chosen * factor, column.shape)
    gain_t = column[pl.ds(pl.multiple_of(lax.rem(me * own, LANES), 8), own), :]
    gain_t = gain_t[:, :1]
    score_ref[...] = found[0] * gain_g * gain_t
    top = jnp.zeros((own, LANES), F32)
    pos = lax.broadcasted_iota(jnp.int32, top.shape, 1)
    for k in range(1, turns):
        peak = jnp.max(jnp.abs(found[k] * gain_g), axis=1, keepdims=True) * gain_t
        top = jnp.where(pos == k - 1, peak, top)
    peaks[0] = top
    crossed = start_all(
        [
            pltpu.make_async_remote_copy(
                src_ref=peaks.at[0],
                dst_ref=peaks.at[d],
                send_sem=tile_send.at[d - 1],
                recv_sem=tile_recv.at[d - 1],
                device_id={"tile": lax.rem(my_tile + d, tiles)},
                device_id_type=MESH,
            )
            for d in range(1, tiles)
        ]
    )
    for copy in scattered + gathered:
        copy.wait_send()

    def finish(k, carry):
        for p in range(n_parts):
            for stage in range(3):
                for copy in copies(k, p, stage):
                    copy.wait_send()
        return carry

    lax.fori_loop(0, turns, finish, 0)
    for d in range(1, groups):
        square_copy(d).wait_send()
    for d in range(1, tiles):
        crossed[d - 1].wait()
        top = jnp.maximum(top, peaks[d])
    peak_ref[...] = top


def scan(traits, covariates, genotypes, shuffles):
    groups, tiles = lax.axis_size("samp"), lax.axis_size("tile")
    dims = grid_of(groups)
    turns = shuffles.shape[0] + 1
    local, n_traits = traits.shape
    width = genotypes.shape[1]
    used = covariates.shape[1] + 1
    own = n_traits // groups
    n_parts = len(ORDERS)
    share = own // n_parts
    bufs = []
    for order in ORDERS:
        left = [0, 1, 2]
        for stage, axis in enumerate(order):
            left.remove(axis)
            rest = tuple(dims[a] for a in left) + (share, width)
            bufs.append(pltpu.VMEM((turns, dims[axis] - 1) + rest, F32))
            if stage < 2:
                bufs.append(pltpu.VMEM((turns,) + rest, F32))
    hops = sum(n - 1 for n in dims)
    rows = -(-(n_traits + width) // (8 * LANES)) * 8
    strips = -(-used // 8)
    quota = -(-strips * ((n_traits + width) // LANES + 1) // groups)
    vmem = pl.BlockSpec(memory_space=pltpu.VMEM)
    sems = pltpu.SemaphoreType.DMA((turns, n_parts, hops))
    flat = pltpu.SemaphoreType.DMA((groups - 1,))
    pair = pltpu.SemaphoreType.DMA((max(tiles - 1, 1),))
    return pl.pallas_call(
        functools.partial(scan_kernel, dims, tiles, local * groups, used),
        out_shape=(
            jax.ShapeDtypeStruct((own, width), F32),
            jax.ShapeDtypeStruct((own, LANES), F32),
        ),
        in_specs=[vmem] * 4,
        out_specs=(vmem, vmem),
        scratch_shapes=[
            pltpu.VMEM((local, LANES), BF16),
            pltpu.VMEM((quota * groups, 8, LANES), F32),
            pltpu.VMEM((groups - 1, quota, 8, LANES), F32),
            pltpu.VMEM((quota, 8, LANES), F32),
            pltpu.VMEM((quota * groups, 8, LANES), F32),
            pltpu.VMEM((LANES, n_traits + width), F32),
            pltpu.VMEM((LANES, n_traits + width), BF16),
            pltpu.VMEM((n_traits, local), BF16),
            pltpu.VMEM((local, width), BF16),
            pltpu.VMEM((local, width), BF16),
            pltpu.VMEM((turns, n_parts) + dims + (share, width), F32),
            pltpu.VMEM((turns, own, width), F32),
            pltpu.VMEM((groups, rows, LANES), F32),
            pltpu.VMEM((LANES, LANES), F32),
            pltpu.VMEM((tiles, own, LANES), F32),
            pltpu.SemaphoreType.DMA((4, groups - 1)),
            flat,
            flat,
            pair,
            pair,
            sems,
            sems,
            *bufs,
        ],
        compiler_params=pltpu.CompilerParams(
            collective_id=0, has_side_effects=True, vmem_limit_bytes=60 * 1024 * 1024
        ),
        name="scan",
    )(traits, covariates, genotypes, shuffles)


def shards(traits, covariates, genotypes, shuffles):
    observed, peaks = scan(traits, covariates, genotypes, shuffles)
    return (observed, peaks[:, : shuffles.shape[0]].T)


def solution(mesh):
    placed = (P("samp", None), P("samp", None), P("samp", "tile"), P(None, "samp"))
    return jax.shard_map(
        shards,
        mesh=mesh,
        in_specs=placed,
        out_specs=(P("samp", "tile"), P(None, "samp")),
        check_vma=False,
    )
```

```python
import functools
import math

import jax
import jax.numpy as jnp
from jax import lax
from jax.experimental import pallas as pl
from jax.experimental.pallas import tpu as pltpu
from jax.sharding import PartitionSpec as P

MESH = pl.DeviceIdType.MESH
LANES = 128
F32, BF16 = jnp.float32, jnp.bfloat16
epsilon = 1e-05

def parts_of(own, width):
    cut, half = own - max(8, own // 64 * 8), width // 2
    return (
        ((2, 1, 0), slice(0, cut), slice(0, half)),
        ((1, 2, 0), slice(0, cut), slice(half, width)),
        ((0, 2, 1), slice(cut, own), slice(0, width)),
    )


def grid_of(groups):
    x = 4 if groups % 32 == 0 else 2
    y = 2
    return (groups // (x * y), y, x)


def start_all(copies):
    for copy in copies:
        copy.start()
    return copies


def scan_kernel(
    dims, tiles, samples, used, areas, t_ref, c_ref, g_ref, order_ref, score_ref, peak_ref,
    design, parts, landed, mine, full, rhs, coef, rt, rg, moved, found, squares, column,
    peaks, sum_sems, sq_send, sq_recv, tile_send, tile_recv, send, recv, *bufs
):
    groups = dims[0] * dims[1] * dims[2]
    me = lax.axis_index("samp")
    my_tile = lax.axis_index("tile")
    here = (me // (dims[1] * dims[2]), lax.rem(me // dims[2], dims[1]), lax.rem(me, dims[2]))
    turns, width, n_parts = found.shape[0], found.shape[2], len(areas)
    local, traits = t_ref.shape
    own = traits // groups
    rows = coef.shape[0]
    quota = parts.shape[0] // groups

    barrier = pltpu.get_barrier_semaphore()
    for d in range(1, groups):
        pl.semaphore_signal(
            barrier, inc=1, device_id={"samp": lax.rem(me + d, groups)}, device_id_type=MESH
        )
    for d in range(1, tiles):
        pl.semaphore_signal(
            barrier, inc=1, device_id={"tile": lax.rem(my_tile + d, tiles)}, device_id_type=MESH
        )

    lane = lax.broadcasted_iota(jnp.int32, design.shape, 1)
    design[...] = jnp.where(lane == used - 1, 1.0, 0.0).astype(BF16)
    design[:, : used - 1] = c_ref[...]
    strips = -(-used // 8)
    design_t = design[...].T[: -(-used // 16) * 16]
    slot = 0
    for block_ref in (t_ref, g_ref, design):
        block = block_ref[...]
        if block.dtype != BF16:
            block = block.astype(F32).astype(BF16)
        block = jnp.dot(design_t, block, preferred_element_type=F32)
        for c in range(block.shape[1] // LANES):
            for r in range(strips):
                parts[slot] = block[8 * r : 8 * r + 8, LANES * c : LANES * c + LANES]
                slot += 1
    for i in range(slot, parts.shape[0]):
        parts[i] = jnp.zeros((8, LANES), F32)
    pl.semaphore_wait(barrier, groups + tiles - 2)

    def sum_copy(d, source, target, stage):
        return pltpu.make_async_remote_copy(
            src_ref=source,
            dst_ref=target,
            send_sem=sum_sems.at[2 * stage, d - 1],
            recv_sem=sum_sems.at[2 * stage + 1, d - 1],
            device_id={"samp": lax.rem(me + d, groups)},
            device_id_type=MESH,
        )

    scattered = start_all(
        [
            sum_copy(
                d, parts.at[pl.ds(lax.rem(me + d, groups) * quota, quota)], landed.at[d - 1], 0
            )
            for d in range(1, groups)
        ]
    )
    total = parts[pl.ds(me * quota, quota)]
    for d in range(1, groups):
        scattered[d - 1].wait_recv()
        total = total + landed[d - 1]
    mine[...] = total
    full[pl.ds(me * quota, quota)] = total
    gathered = start_all(
        [sum_copy(d, mine, full.at[pl.ds(me * quota, quota)], 1) for d in range(1, groups)]
    )
    rhs[...] = jnp.zeros(rhs.shape, F32)
    for copy in gathered:
        copy.wait_recv()

    n_t, n_g = traits // LANES, width // LANES
    half = rows // 2
    for c in range(n_t + n_g):
        for r in range(strips):
            rhs[half + 8 * r : half + 8 * r + 8, LANES * c : LANES * c + LANES] = full[
                c * strips + r
            ]
    gram = jnp.concatenate([full[(n_t + n_g) * strips + r] for r in range(strips)], axis=0)
    sub = lax.broadcasted_iota(jnp.int32, gram.shape, 0)
    lane = lax.broadcasted_iota(jnp.int32, gram.shape, 1)
    gram = jnp.where(lane == sub + half, 1.0, gram)
    for j in range(used):
        row = gram[j : j + 1, :] * (1.0 / gram[j : j + 1, j : j + 1])
        gram = jnp.where(sub == j, row, gram - gram[:, j : j + 1] * row)
    inverse = jnp.where(lane >= half, gram, 0.0)
    coef[...] = jnp.zeros(coef.shape, BF16)
    coef[: 8 * strips, :] = jnp.dot(
        inverse, rhs[...], precision=lax.Precision.HIGHEST, preferred_element_type=F32
    ).astype(BF16)

    step = min(256, local)
    sq_t = jnp.zeros((1, traits), F32)
    sq_g = jnp.zeros((1, width), F32)
    for i in range(local // step):
        at = slice(i * step, (i + 1) * step)
        d = design[at, :]
        resid = t_ref[at, :].astype(F32) - jnp.dot(
            d, coef[:, :traits], preferred_element_type=F32
        )
        sq_t = sq_t + jnp.sum(resid * resid, axis=0, keepdims=True)
        rt[:, at] = resid.astype(BF16).T
        dose = g_ref[at, :].astype(F32)
        resid = dose - jnp.dot(d, coef[:, traits:], preferred_element_type=F32)
        sq_g = sq_g + jnp.sum(resid * resid, axis=0, keepdims=True)
        rg[at, :] = resid.astype(BF16)
    squares[0] = jnp.zeros(squares.shape[1:], F32)
    for c in range(n_t):
        squares[0, c : c + 1, :] = sq_t[:, c * LANES : (c + 1) * LANES]
    for c in range(n_g):
        squares[0, n_t + c : n_t + c + 1, :] = sq_g[:, c * LANES : (c + 1) * LANES]

    def square_copy(d):
        return pltpu.make_async_remote_copy(
            src_ref=squares.at[0],
            dst_ref=squares.at[d],
            send_sem=sq_send.at[d - 1],
            recv_sem=sq_recv.at[d - 1],
            device_id={"samp": lax.rem(me + d, groups)},
            device_id_type=MESH,
        )

    def spot(axis, d):
        j = lax.rem(here[axis] + d, dims[axis])
        at = list(here)
        at[axis] = j
        return j, (at[0] * dims[1] + at[1]) * dims[2] + at[2]

    def pick(axis, order, stage, j):
        left = [a for a in (0, 1, 2) if a not in order[:stage]]
        return tuple(j if a == axis else slice(None) for a in left)

    def source(k, p, stage):
        return bufs[6 * p + 2 * stage].at[k]

    def copies(k, p, stage):
        order = areas[p][0]
        axis = order[stage]
        first = sum(dims[a] - 1 for a in order[:stage])
        out = []
        for d in range(1, dims[axis]):
            j, peer = spot(axis, d)
            out.append(
                pltpu.make_async_remote_copy(
                    src_ref=source(k, p, stage).at[pick(axis, order, stage, j)],
                    dst_ref=bufs[6 * p + 2 * stage + 1].at[k, d - 1],
                    send_sem=send.at[k, p, first + d - 1],
                    recv_sem=recv.at[k, p, first + d - 1],
                    device_id={"samp": peer},
                    device_id_type=MESH,
                )
            )
        return out

    def begin(k, stage):
        for p in range(n_parts):
            for copy in copies(k, p, stage):
                copy.start()

    def collect(k, stage):
        for p in range(n_parts):
            order = areas[p][0]
            axis = order[stage]
            for copy in copies(k, p, stage):
                copy.wait_recv()
            total = source(k, p, stage)[pick(axis, order, stage, here[axis])]
            for d in range(1, dims[axis]):
                total = total + bufs[6 * p + 2 * stage + 1][k, d - 1]
            if stage < 2:
                bufs[6 * p + 2 * stage + 2][k] = total
            else:
                found[k, areas[p][1], areas[p][2]] = total

    def multiply(k):
        @pl.when(k == 0)
        def _():
            moved[...] = rg[...]

        @pl.when(k > 0)
        def _():
            order = order_ref[pl.ds(k - 1, 1), :] - me * local
            for i in range(local // step):
                row = lax.broadcasted_iota(jnp.int32, (step, local), 0) + i * step
                hot = jnp.where(row == order, 1.0, 0.0).astype(BF16)
                moved[i * step : (i + 1) * step, :] = jnp.dot(
                    hot, rg[...], preferred_element_type=F32
                ).astype(BF16)

        depth = traits // dims[0]
        for z in range(dims[0]):
            block = jnp.dot(
                rt[z * depth : (z + 1) * depth, :], moved[...], preferred_element_type=F32
            ).reshape(dims[1], dims[2], own, width)
            for p in range(n_parts):
                bufs[6 * p][k, z] = block[:, :, areas[p][1], areas[p][2]]

    def turn(t, carry):
        @pl.when(t < turns)
        def _():
            multiply(t)
            begin(t, 0)

        @pl.when(t == 0)
        def _():
            for d in range(1, groups):
                square_copy(d).start()

        for stage in range(3):
            k = t - 1 - stage

            @pl.when(jnp.logical_and(k >= 0, k < turns))
            def _():
                collect(k, stage)
                if stage < 2:
                    begin(k, stage + 1)

        return carry

    lax.fori_loop(0, turns + 3, turn, 0)

    total = squares[0]
    for d in range(1, groups):
        square_copy(d).wait_recv()
        total = total + squares[d]
    gain = lax.rsqrt(total / samples + epsilon)
    factor = math.sqrt(samples - used - 1) / samples
    gain_g = jnp.concatenate([gain[n_t + c : n_t + c + 1, :] for c in range(n_g)], axis=1)
    turned = gain.T
    pos = lax.broadcasted_iota(jnp.int32, turned.shape, 1)
    chosen = jnp.sum(
        jnp.where(pos == me * own // LANES, turned, 0.0), axis=1, keepdims=True
    )
    column[...] = jnp.broadcast_to(chosen * factor, column.shape)
    gain_t = column[pl.ds(pl.multiple_of(lax.rem(me * own, LANES), 8), own), :]
    gain_t = gain_t[:, :1]
    score_ref[...] = found[0] * gain_g * gain_t
    top = jnp.zeros((own, LANES), F32)
    pos = lax.broadcasted_iota(jnp.int32, top.shape, 1)
    for k in range(1, turns):
        peak = jnp.max(jnp.abs(found[k] * gain_g), axis=1, keepdims=True) * gain_t
        top = jnp.where(pos == k - 1, peak, top)
    peaks[0] = top
    crossed = start_all(
        [
            pltpu.make_async_remote_copy(
                src_ref=peaks.at[0],
                dst_ref=peaks.at[d],
                send_sem=tile_send.at[d - 1],
                recv_sem=tile_recv.at[d - 1],
                device_id={"tile": lax.rem(my_tile + d, tiles)},
                device_id_type=MESH,
            )
            for d in range(1, tiles)
        ]
    )
    for copy in scattered + gathered:
        copy.wait_send()

    def finish(k, carry):
        for p in range(n_parts):
            for stage in range(3):
                for copy in copies(k, p, stage):
                    copy.wait_send()
        return carry

    lax.fori_loop(0, turns, finish, 0)
    for d in range(1, groups):
        square_copy(d).wait_send()
    for d in range(1, tiles):
        crossed[d - 1].wait()
        top = jnp.maximum(top, peaks[d])
    peak_ref[...] = top.T[: turns - 1]


def scan(traits, covariates, genotypes, shuffles):
    groups, tiles = lax.axis_size("samp"), lax.axis_size("tile")
    dims = grid_of(groups)
    turns = shuffles.shape[0] + 1
    local, n_traits = traits.shape
    width = genotypes.shape[1]
    used = covariates.shape[1] + 1
    own = n_traits // groups
    areas = parts_of(own, width)
    n_parts = len(areas)
    bufs = []
    for order, part_rows, part_lanes in areas:
        size = (part_rows.stop - part_rows.start, part_lanes.stop - part_lanes.start)
        left = [0, 1, 2]
        bufs.append(pltpu.VMEM((turns,) + dims + size, F32))
        for stage, axis in enumerate(order):
            left.remove(axis)
            rest = tuple(dims[a] for a in left) + size
            bufs.append(pltpu.VMEM((turns, dims[axis] - 1) + rest, F32))
            if stage < 2:
                bufs.append(pltpu.VMEM((turns,) + rest, F32))
    hops = sum(n - 1 for n in dims)
    rows = -(-(n_traits + width) // (8 * LANES)) * 8
    strips = -(-used // 8)
    quota = -(-strips * ((n_traits + width) // LANES + 1) // groups)
    vmem = pl.BlockSpec(memory_space=pltpu.VMEM)
    sems = pltpu.SemaphoreType.DMA((turns, n_parts, hops))
    flat = pltpu.SemaphoreType.DMA((groups - 1,))
    pair = pltpu.SemaphoreType.DMA((max(tiles - 1, 1),))
    return pl.pallas_call(
        functools.partial(scan_kernel, dims, tiles, local * groups, used, areas),
        out_shape=(
            jax.ShapeDtypeStruct((own, width), F32),
            jax.ShapeDtypeStruct((turns - 1, own), F32),
        ),
        in_specs=[vmem] * 4,
        out_specs=(vmem, vmem),
        scratch_shapes=[
            pltpu.VMEM((local, LANES), BF16),
            pltpu.VMEM((quota * groups, 8, LANES), F32),
            pltpu.VMEM((groups - 1, quota, 8, LANES), F32),
            pltpu.VMEM((quota, 8, LANES), F32),
            pltpu.VMEM((quota * groups, 8, LANES), F32),
            pltpu.VMEM((LANES, n_traits + width), F32),
            pltpu.VMEM((LANES, n_traits + width), BF16),
            pltpu.VMEM((n_traits, local), BF16),
            pltpu.VMEM((local, width), BF16),
            pltpu.VMEM((local, width), BF16),
            pltpu.VMEM((turns, own, width), F32),
            pltpu.VMEM((groups, rows, LANES), F32),
            pltpu.VMEM((LANES, LANES), F32),
            pltpu.VMEM((tiles, own, LANES), F32),
            pltpu.SemaphoreType.DMA((4, groups - 1)),
            flat,
            flat,
            pair,
            pair,
            sems,
            sems,
            *bufs,
        ],
        compiler_params=pltpu.CompilerParams(
            collective_id=0, has_side_effects=True, vmem_limit_bytes=60 * 1024 * 1024
        ),
        name="scan",
    )(traits, covariates, genotypes, shuffles)


def shards(traits, covariates, genotypes, shuffles):
    return scan(traits, covariates, genotypes, shuffles)


def solution(mesh):
    placed = (P("samp", None), P("samp", None), P("samp", "tile"), P(None, "samp"))
    return jax.shard_map(
        shards,
        mesh=mesh,
        in_specs=placed,
        out_specs=(P("samp", "tile"), P(None, "samp")),
        check_vma=False,
    )
```
